32 devices in a mesh: section: 2 (over core), dp: 4 (over y, x), tensor: 4 (over z).
Axes of the slice: x: 2, y: 2, z: 4, core: 2. Of those that a mesh axis runs over, the one named last changes fastest.
Arguments:
- tokens_in: bfloat16 [512, 8192], P('dp', ('section', 'tensor')), may hold values from -70 to 70
- gain_attn: bfloat16 [8192], replicated, may hold values from 0.5 to 1.5
- w_query: bfloat16 [8192, 8192], P(None, ('section', 'tensor')), may hold values from -6 to 6
- w_keyval: bfloat16 [8192, 2048], P(None, ('section', 'tensor')), may hold values from -0.0625 to 0.0625
- w_out: bfloat16 [8192, 8192], P(('section', 'tensor')), may hold values from -0.0625 to 0.0625
- gain_mlp: bfloat16 [8192], replicated, may hold values from 0.5 to 1.5
- w_gate: bfloat16 [8192, 16384], P('dp', ('section', 'tensor')), may hold values from -0.0625 to 0.0625
- w_up: bfloat16 [8192, 16384], P('dp', ('section', 'tensor')), may hold values from -0.0625 to 0.0625
- w_down: bfloat16 [16384, 8192], P(('section', 'tensor'), 'dp'), may hold values from -0.046875 to 0.046875
Outputs:
- layer_out: bfloat16 [512, 8192], P(('section', 'tensor'), 'dp')
The draws below stay inside these ranges and needn't reach their ends.
All inputs are finite; a program needn't handle non-finite values.
Results may differ from the reference program's by a relative error of at most 0.0068.
Values may be sent and summed in bfloat16 or wider, within the bound.
A program may use at most 128 MiB of HBM per device.

```python
import math
import jax
import jax.numpy as jnp
from jax import lax

D = 8192
H = 64
KVH = 8
HD = 128
FF = 16384
TOKENS = 512


def draw_tokens_in(key, part):
    first_key, scale_key = jax.random.split(jax.random.fold_in(key, 11), 2)
    base_values = jnp.clip(jax.random.normal(first_key, (TOKENS, D), jnp.float32), -6.0, 6.0)
    scales = jnp.exp(jax.random.uniform(scale_key, (TOKENS, 1), jnp.float32, math.log(0.3), math.log(3.0)))
    values = scales * base_values
    return values.astype(jnp.bfloat16)


def draw_w_query(key, part):
    entry_key, head_key = jax.random.split(jax.random.fold_in(key, 23), 2)
    base_values = jnp.clip(jax.random.normal(entry_key, (D, H * HD), jnp.float32), -6.0, 6.0) * D ** (-0.5)
    head_scale = jnp.exp(jax.random.uniform(head_key, (H,), jnp.float32, 0.0, math.log(3.0)))
    values = base_values * jnp.repeat(head_scale, HD)[None, :]
    values = jnp.clip(values, -6.0, 6.0)
    return values.astype(jnp.bfloat16)


def block_levels(own_key, extent, pieces, smallest, high):
    factor_of = 1.0
    for dim, parts in pieces:
        steps = jax.random.uniform(jax.random.fold_in(jax.random.fold_in(own_key, 6), dim), (parts,), jnp.float32, smallest / len(pieces), high / len(pieces))
        factor_of = factor_of * jnp.repeat(jnp.exp(steps), extent[dim] // parts).reshape((-1,) + (1,) * (len(extent) - 1 - dim))
    return factor_of


def noise(stream_key, dims, width, limit, shards=(), kind=jnp.bfloat16):
    entries = width * jax.random.normal(stream_key, dims, jnp.float32)
    if shards:
        entries = entries * block_levels(stream_key, dims, shards, -0.22, 0.18)
    return jnp.clip(entries, -limit, limit).astype(kind)


def setup_inputs(seed: int = 0) -> dict:
    arg_keys = jax.random.split(jax.random.key(seed), 10)
    tokens_in = draw_tokens_in(jax.random.fold_in(arg_keys[9], 71), 0)
    gain_attn = jnp.clip(1.0 + 0.1 * jax.random.normal(arg_keys[1], (D,), jnp.float32), 0.5, 1.5).astype(jnp.bfloat16)
    w_query = draw_w_query(jax.random.fold_in(arg_keys[9], 71), 0)
    w_keyval = noise(arg_keys[3], (D, 2 * KVH * HD), D ** -0.5, 0.0625, ((1, 8),))
    w_out = noise(arg_keys[4], (H * HD, D), (H * HD) ** -0.5, 0.0625, ((0, 8),))
    gain_mlp = jnp.clip(1.0 + 0.1 * jax.random.normal(arg_keys[5], (D,), jnp.float32), 0.5, 1.5).astype(jnp.bfloat16)
    w_gate = noise(arg_keys[6], (D, FF), D ** -0.5, 0.0625, ((0, 4), (1, 8)))
    w_up = noise(arg_keys[7], (D, FF), D ** -0.5, 0.0625, ((0, 4), (1, 8)))
    w_down = noise(arg_keys[8], (FF, D), FF ** -0.5, 0.046875, ((0, 8), (1, 4)))
    return {"tokens_in": tokens_in, "gain_attn": gain_attn, "w_query": w_query, "w_keyval": w_keyval, "w_out": w_out, "gain_mlp": gain_mlp, "w_gate": w_gate, "w_up": w_up, "w_down": w_down}


EPS = 1e-05
THETA = 10000.0

def rms_scale(row_data, gain_row):
    values = row_data.astype(jnp.float32)
    factor = lax.rsqrt(lax.optimization_barrier(jnp.mean(values * values, axis=-1, keepdims=True)) + EPS)
    return (values * factor * gain_row.astype(jnp.float32)).astype(jnp.bfloat16)

def rotary(values, positions):
    half_dim = values.shape[-1] // 2
    frequency = THETA ** (-jnp.arange(half_dim, dtype=jnp.float32) * 2.0 / values.shape[-1])
    angles = positions.astype(jnp.float32)[:, None] * frequency[None, :]
    cosine = jnp.cos(angles)[:, None, :]
    sine_part = jnp.sin(angles)[:, None, :]
    first_half = values[..., :half_dim]
    second = values[..., half_dim:]
    return jnp.concatenate([first_half * cosine - second * sine_part, second * cosine + first_half * sine_part], axis=-1)

def reference(tokens_in, gain_attn, w_query, w_keyval, w_out, gain_mlp, w_gate, w_up, w_down):
    total_rows = tokens_in.shape[0]
    normed_attn = rms_scale(tokens_in, gain_attn)
    positions = jnp.arange(total_rows, dtype=jnp.int32)
    query_proj = jnp.dot(normed_attn, w_query, preferred_element_type=jnp.float32)
    query_rot = rotary(query_proj.reshape(total_rows, H, HD), positions).astype(jnp.bfloat16)
    keyval = jnp.dot(normed_attn, w_keyval, preferred_element_type=jnp.float32).astype(jnp.bfloat16)
    key_rot = rotary(keyval[:, :KVH * HD].astype(jnp.float32).reshape(total_rows, KVH, HD), positions).astype(jnp.bfloat16)
    value_all = keyval[:, KVH * HD:].reshape(total_rows, KVH, HD)
    group_size = H // KVH
    query_grp = query_rot.reshape(total_rows, KVH, group_size, HD)
    allowed = positions[None, :] <= positions[:, None]

    def one_group(operands):
        q_block, k_block, v_block = operands
        scores = jnp.einsum('rgd,sd->grs', q_block.astype(jnp.float32), k_block.astype(jnp.float32)) * HD ** (-0.5)
        scores = jnp.where(allowed[None, :, :], scores, -1e+30)
        row_peak = lax.optimization_barrier(jnp.max(scores, axis=-1, keepdims=True))
        expo = jnp.exp(scores - row_peak)
        prob_rows = (expo / lax.optimization_barrier(jnp.sum(expo, axis=-1, keepdims=True))).astype(jnp.bfloat16)
        mixed = jnp.einsum('grs,sd->rgd', prob_rows.astype(jnp.float32), v_block.astype(jnp.float32))
        return mixed.astype(jnp.bfloat16)
    attended = lax.map(one_group, (jnp.transpose(query_grp, (1, 0, 2, 3)), jnp.transpose(key_rot, (1, 0, 2)), jnp.transpose(value_all, (1, 0, 2))))
    attended = jnp.transpose(attended, (1, 0, 2, 3)).reshape(total_rows, H * HD)
    head_sum = jnp.dot(attended, w_out, preferred_element_type=jnp.float32)
    mid_rows = (tokens_in.astype(jnp.float32) + head_sum).astype(jnp.bfloat16)
    normed_mlp = rms_scale(mid_rows, gain_mlp)
    gate_sum = jnp.dot(normed_mlp, w_gate, preferred_element_type=jnp.float32)
    up_sum = jnp.dot(normed_mlp, w_up, preferred_element_type=jnp.float32)
    hidden = (jax.nn.silu(gate_sum) * up_sum).astype(jnp.bfloat16)
    down_sum = jnp.dot(hidden, w_down, preferred_element_type=jnp.float32)
    return (mid_rows.astype(jnp.float32) + down_sum).astype(jnp.bfloat16)
```

```python
import functools

import jax
import jax.numpy as jnp
from jax import lax
from jax.experimental import pallas as pl
from jax.experimental.pallas import tpu as pltpu
from jax.sharding import PartitionSpec as P

H = 64
KVH = 8
HD = 128
EPS = 1e-05
THETA = 10000.0
CHUNKS = 4
MESH = pl.DeviceIdType.MESH
F32 = jnp.float32
BF16 = jnp.bfloat16
VMEM = pl.BlockSpec(memory_space=pltpu.VMEM)
ANY = pl.BlockSpec(memory_space=pl.ANY)


def rms_scale(row_data, gain_row):
    values = row_data.astype(jnp.float32)
    factor = lax.rsqrt(jnp.mean(values * values, axis=-1, keepdims=True) + EPS)
    return (values * factor * gain_row.astype(jnp.float32)).astype(jnp.bfloat16)


def rotary(values, positions):
    half_dim = values.shape[-1] // 2
    frequency = THETA ** (-jnp.arange(half_dim, dtype=jnp.float32) * 2.0 / values.shape[-1])
    angles = positions.astype(jnp.float32)[:, None] * frequency[None, :]
    cosine = jnp.cos(angles)[:, None, :]
    sine_part = jnp.sin(angles)[:, None, :]
    first_half = values[..., :half_dim]
    second = values[..., half_dim:]
    return jnp.concatenate(
        [first_half * cosine - second * sine_part, second * cosine + first_half * sine_part],
        axis=-1,
    )


def greet(peers):
    barrier = pltpu.get_barrier_semaphore()
    for peer in peers:
        pl.semaphore_signal(barrier, inc=1, device_id=peer, device_id_type=MESH)
    pl.semaphore_wait(barrier, len(peers))


def push(src, dst, sems, slot, device):
    return pltpu.make_async_remote_copy(
        src_ref=src,
        dst_ref=dst,
        send_sem=sems.at[0, slot],
        recv_sem=sems.at[1, slot],
        device_id=device,
        device_id_type=MESH,
    )


def others(axis):
    size = lax.axis_size(axis)
    me = lax.axis_index(axis)
    return [(step, lax.rem(me + step, size), lax.rem(me + size - step, size)) for step in range(1, size)]


def gather_group(out, at, sem_t, sem_s):
    section, tensor = lax.axis_index("section"), lax.axis_index("tensor")
    sections, tensors = others("section"), others("tensor")
    size_t = lax.axis_size("tensor")
    started = []

    def pass_on(block_t, slot):
        for step, to, _ in sections:
            block = out.at[at(section, block_t)]
            copy = push(block, block, sem_s, slot * len(sections) + step - 1, {"section": to})
            copy.start()
            started.append(copy)

    for step, to, _ in tensors:
        block = out.at[at(section, tensor)]
        copy = push(block, block, sem_t, step - 1, {"tensor": to})
        copy.start()
        started.append(copy)
    pass_on(tensor, 0)
    for step, to, source in tensors:
        block = out.at[at(section, source)]
        push(block, block, sem_t, step - 1, {"tensor": to}).wait_recv()
        pass_on(source, step)
    for slot in range(size_t):
        for step, to, source in sections:
            source_t = lax.rem(tensor + size_t - slot, size_t)
            block = out.at[at(source, source_t)]
            push(block, block, sem_s, slot * len(sections) + step - 1, {"section": to}).wait_recv()
    for copy in started:
        copy.wait_send()


def group_peers():
    return [{"tensor": to} for _, to, _ in others("tensor")] + [
        {"section": to} for _, to, _ in others("section")
    ]


def dma_sems(count):
    return pltpu.SemaphoreType.DMA((2, max(1, count)))


def ag_group_body(x_ref, out_ref, sem_t, sem_s, sem_local):
    section, tensor = lax.axis_index("section"), lax.axis_index("tensor")
    size_t = lax.axis_size("tensor")
    greet(group_peers())
    own = pltpu.make_async_copy(x_ref, out_ref.at[section * size_t + tensor], sem_local)
    own.start()
    own.wait()
    gather_group(out_ref, lambda s, t: s * size_t + t, sem_t, sem_s)


def ag_group(x, collective_id):
    size_s, size_t = lax.axis_size("section"), lax.axis_size("tensor")
    return pl.pallas_call(
        ag_group_body,
        out_shape=jax.ShapeDtypeStruct((size_s * size_t,) + x.shape, x.dtype),
        in_specs=[VMEM],
        out_specs=VMEM,
        scratch_shapes=[dma_sems(size_t - 1), dma_sems(size_t * (size_s - 1)), pltpu.SemaphoreType.DMA],
        compiler_params=pltpu.CompilerParams(collective_id=collective_id, has_side_effects=True),
    )(x)


def ag_dp_body(x_ref, out_ref, sem_d, sem_local):
    me = lax.axis_index("dp")
    greet([{"dp": to} for _, to, _ in others("dp")])
    own = pltpu.make_async_copy(x_ref, out_ref.at[me], sem_local)
    own.start()
    copies = []
    for step, to, _ in others("dp"):
        copy = push(x_ref, out_ref.at[me], sem_d, step - 1, {"dp": to})
        copy.start()
        copies.append(copy)
    own.wait()
    for step, to, source in others("dp"):
        push(x_ref, out_ref.at[source], sem_d, step - 1, {"dp": to}).wait_recv()
    for copy in copies:
        copy.wait_send()


def ag_dp(x, collective_id):
    size_d = lax.axis_size("dp")
    return pl.pallas_call(
        ag_dp_body,
        out_shape=jax.ShapeDtypeStruct((size_d,) + x.shape, x.dtype),
        in_specs=[VMEM],
        out_specs=VMEM,
        scratch_shapes=[dma_sems(size_d - 1), pltpu.SemaphoreType.DMA],
        compiler_params=pltpu.CompilerParams(collective_id=collective_id, has_side_effects=True),
    )(x)


def tile_of(width, most):
    return width if width <= most else most


def scatter_group(part, pair_rx, comb, z_rx, sem_p, sem_z):
    section, tensor = lax.axis_index("section"), lax.axis_index("tensor")
    size_t = lax.axis_size("tensor")
    block = z_rx.shape[1]

    def rows(s, t):
        return pl.ds(pl.multiple_of((s * size_t + t) * block, block), block)

    sections, tensors = others("section"), others("tensor")
    order = [(step, to) for step, to, _ in tensors] + [(0, tensor)]
    started = []
    for step, to in order:
        for hop, other, _ in sections:
            copy = push(
                part.at[rows(other, to)],
                pair_rx.at[hop - 1, step],
                sem_p,
                (hop - 1) * size_t + step,
                {"section": other},
            )
            copy.start()
            started.append(copy)

    def paired(step, to):
        total = part[rows(section, to), :].astype(F32)
        for hop, other, _ in sections:
            push(
                part.at[rows(other, to)],
                pair_rx.at[hop - 1, step],
                sem_p,
                (hop - 1) * size_t + step,
                {"section": other},
            ).wait_recv()
            total = total + pair_rx[hop - 1, step].astype(F32)
        return total

    for step, to, _ in tensors:
        comb[step - 1] = paired(step, to).astype(BF16)
        copy = push(comb.at[step - 1], z_rx.at[step - 1], sem_z, step - 1, {"tensor": to})
        copy.start()
        started.append(copy)
    total = paired(0, tensor)
    for step, to, _ in tensors:
        push(comb.at[step - 1], z_rx.at[step - 1], sem_z, step - 1, {"tensor": to}).wait_recv()
        total = total + z_rx[step - 1].astype(F32)
    for copy in started:
        copy.wait_send()
    return total


def back_body(
    att_ref, rows_ref, gain_ref, wo_hbm, wg_hbm, wu_hbm, wd_hbm, out_ref,
    wo, wg, wu, wd, att_all, part, pair_rx, comb, z_rx, resid, mid, stat_tx, stat_rx,
    nrm, gu, rx1, tx2, rx2, hid, acc, part2, pair_rx2, comb2, z_rx2,
    sem_w, sem_own, sem_att, sem_res, sem_p, sem_z, sem_stat, sem_t, sem_s,
    sem_1, sem_2, sem_h, sem_p2, sem_z2,
):
    section, tensor, me = lax.axis_index("section"), lax.axis_index("tensor"), lax.axis_index("dp")
    size_t, size_d = lax.axis_size("tensor"), lax.axis_size("dp")
    group_index = section * size_t + tensor
    local_rows, width = att_ref.shape
    block, cols = mid.shape
    total_rows = att_all.shape[0]
    features = rows_ref.shape[1]
    dps = others("dp")
    sends = []

    loads = [
        pltpu.make_async_copy(wo_hbm.at[:, pl.ds(pl.multiple_of(me * cols, cols), cols)], wo, sem_w.at[0]),
        pltpu.make_async_copy(wg_hbm, wg, sem_w.at[1]),
        pltpu.make_async_copy(wu_hbm, wu, sem_w.at[2]),
        pltpu.make_async_copy(wd_hbm, wd, sem_w.at[3]),
    ]
    for load in loads:
        load.start()

    greet(group_peers() + [{"dp": to} for _, to, _ in dps])

    def dp_rows(index):
        return pl.ds(pl.multiple_of(index * local_rows, local_rows), local_rows)

    for step, to, _ in dps:
        copy = push(att_ref, att_all.at[dp_rows(me)], sem_att, step - 1, {"dp": to})
        copy.start()
        sends.append(copy)

    per = local_rows // block
    holder = group_index // per
    held_rows = pl.ds(pl.multiple_of(lax.rem(group_index, per) * block, block), block)

    def resid_copy(step, to):
        src = rows_ref.at[held_rows, pl.ds(pl.multiple_of(to * cols, cols), cols)]
        return push(src, resid, sem_res, step - 1, {"dp": to})

    @pl.when(me == holder)
    def _():
        for step, to, _ in dps:
            resid_copy(step, to).start()
        resid[...] = rows_ref[held_rows, pl.ds(pl.multiple_of(me * cols, cols), cols)]

    att_all[dp_rows(me), :] = att_ref[...]
    loads[0].wait()
    tile = tile_of(cols, 512)

    def out_part(index):
        lines = att_all[dp_rows(index), :]

        @pl.loop(0, cols // tile)
        def _(j):
            at = pl.ds(pl.multiple_of(j * tile, tile), tile)
            part[dp_rows(index), at] = jnp.dot(lines, wo[:, at], preferred_element_type=F32).astype(BF16)

    out_part(me)
    for step, to, source in dps:
        push(att_ref, att_all.at[dp_rows(source)], sem_att, step - 1, {"dp": to}).wait_recv()
        out_part(source)

    summed = scatter_group(part, pair_rx, comb, z_rx, sem_p, sem_z)

    for step, to, source in dps:
        @pl.when(source == holder)
        def _():
            resid_copy(step, to).wait_recv()

    @pl.when(me == holder)
    def _():
        for step, to, _ in dps:
            resid_copy(step, to).wait_send()

    mid_rows = (resid[...].astype(F32) + summed).astype(BF16)
    mid[...] = mid_rows
    squares = mid_rows.astype(F32)
    stat = jnp.sum(squares * squares, axis=-1, keepdims=True)
    stat_tx[...] = jnp.broadcast_to(stat, stat_tx.shape)
    for step, to, _ in dps:
        copy = push(stat_tx, stat_rx.at[step - 1], sem_stat, step - 1, {"dp": to})
        copy.start()
        sends.append(copy)
    for step, to, _ in dps:
        push(stat_tx, stat_rx.at[step - 1], sem_stat, step - 1, {"dp": to}).wait_recv()
        stat = stat + stat_rx[step - 1][:, :1]
    factor = lax.rsqrt(stat * (1.0 / features) + EPS)

    def token_rows(s, t):
        return pl.ds(pl.multiple_of((s * size_t + t) * block, block), block)

    nrm[token_rows(section, tensor), :] = (
        mid[...].astype(F32) * factor * gain_ref[...].astype(F32)
    ).astype(BF16)
    gather_group(nrm, token_rows, sem_t, sem_s)

    loads[1].wait()
    loads[2].wait()
    share = gu.shape[2] // 2
    gtile = tile_of(share, 256)
    square = size_d == 4
    if square:
        x, y = lax.rem(me, 2), me // 2
        near = [y * 2 + (1 - x), (1 - y) * 2 + x]
        far = (1 - y) * 2 + (1 - x)
    for c in range(CHUNKS):
        @pl.loop(0, share // gtile)
        def _(j):
            src = pl.ds(pl.multiple_of(c * share + j * gtile, gtile), gtile)
            lo = pl.ds(pl.multiple_of(j * gtile, gtile), gtile)
            hi = pl.ds(pl.multiple_of(share + j * gtile, gtile), gtile)
            gu[c, :, lo] = jnp.dot(nrm[...], wg[:, src], preferred_element_type=F32).astype(BF16)
            gu[c, :, hi] = jnp.dot(nrm[...], wu[:, src], preferred_element_type=F32).astype(BF16)

        if square:
            first = near[c % 2]
            for slot, owner in ((1, far), (0, first)):
                copy = push(gu.at[c, dp_rows(owner)], rx1.at[c, slot], sem_1, 2 * c + slot, {"dp": first})
                copy.start()
                sends.append(copy)
        else:
            for step, to, _ in dps:
                slot = step - 1
                copy = push(gu.at[c, dp_rows(to)], rx1.at[c, slot], sem_1, (size_d - 1) * c + slot, {"dp": to})
                copy.start()
                sends.append(copy)

    if square:
        for c in range(CHUNKS):
            first, second = near[c % 2], near[1 - c % 2]
            push(gu.at[c, dp_rows(far)], rx1.at[c, 1], sem_1, 2 * c + 1, {"dp": first}).wait_recv()
            tx2[c] = (gu[c, dp_rows(second), :].astype(F32) + rx1[c, 1].astype(F32)).astype(BF16)
            copy = push(tx2.at[c], rx2.at[c], sem_2, c, {"dp": second})
            copy.start()
            sends.append(copy)

    hid_slots = size_d - 1
    for c in range(CHUNKS):
        both = gu[c, dp_rows(me), :].astype(F32)
        if square:
            first, second = near[c % 2], near[1 - c % 2]
            push(gu.at[c, dp_rows(first)], rx1.at[c, 0], sem_1, 2 * c, {"dp": first}).wait_recv()
            push(tx2.at[c], rx2.at[c], sem_2, c, {"dp": second}).wait_recv()
            both = both + rx1[c, 0].astype(F32) + rx2[c].astype(F32)
        else:
            for step, to, _ in dps:
                slot = step - 1
                push(
                    gu.at[c, dp_rows(to)], rx1.at[c, slot], sem_1, (size_d - 1) * c + slot, {"dp": to}
                ).wait_recv()
                both = both + rx1[c, slot].astype(F32)
        gate, up = both[:, :share], both[:, share:]
        hid[c, dp_rows(me), :] = (gate / (1.0 + jnp.exp(-gate)) * up).astype(BF16)
        mine = hid.at[c, dp_rows(me)]
        targets = list(enumerate(near)) if square else [(step - 1, to) for step, to, _ in dps]
        for slot, to in targets:
            copy = push(mine, mine, sem_h, hid_slots * c + slot, {"dp": to})
            copy.start()
            sends.append(copy)

    if square:
        for c in range(CHUNKS):
            one, two = c % 2, 1 - c % 2
            theirs = hid.at[c, dp_rows(near[one])]
            push(theirs, theirs, sem_h, hid_slots * c + one, {"dp": near[one]}).wait_recv()
            copy = push(theirs, theirs, sem_h, hid_slots * c + 2, {"dp": near[two]})
            copy.start()
            sends.append(copy)

    loads[3].wait()
    for c in range(CHUNKS):
        if square:
            two = 1 - c % 2
            arrivals = [(two, near[two]), (2, far)]
        else:
            arrivals = [(step - 1, source) for step, _, source in dps]
        for slot, source in arrivals:
            theirs = hid.at[c, dp_rows(source)]
            push(theirs, theirs, sem_h, hid_slots * c + slot, {"dp": source}).wait_recv()

        @pl.loop(0, cols // tile)
        def _(j):
            at = pl.ds(pl.multiple_of(j * tile, tile), tile)
            term = jnp.dot(hid[c], wd[c * share : (c + 1) * share, at], preferred_element_type=F32)
            if c > 0:
                term = acc[:, at] + term
            if c < CHUNKS - 1:
                acc[:, at] = term
            else:
                part2[:, at] = term.astype(BF16)

    total = scatter_group(part2, pair_rx2, comb2, z_rx2, sem_p2, sem_z2)
    out_ref[...] = (mid[...].astype(F32) + total).astype(BF16)
    for copy in sends:
        copy.wait_send()


def back(attended, full_rows, gain, w_out, w_gate, w_up, w_down, collective_id):
    size_s, size_t, size_d = lax.axis_size("section"), lax.axis_size("tensor"), lax.axis_size("dp")
    local_rows, width = attended.shape
    total_rows = local_rows * size_d
    block = total_rows // (size_s * size_t)
    cols, hidden = w_gate.shape
    share = hidden // CHUNKS
    slots = 2 if size_d == 4 else size_d - 1
    scatter = [
        pltpu.VMEM((total_rows, cols), BF16),
        pltpu.VMEM((size_s - 1, size_t, block, cols), BF16),
        pltpu.VMEM((size_t - 1, block, cols), BF16),
        pltpu.VMEM((size_t - 1, block, cols), BF16),
    ]
    return pl.pallas_call(
        back_body,
        out_shape=jax.ShapeDtypeStruct((block, cols), BF16),
        in_specs=[VMEM, VMEM, VMEM, ANY, ANY, ANY, ANY],
        out_specs=VMEM,
        scratch_shapes=[
            pltpu.VMEM((width, cols), BF16),
            pltpu.VMEM(w_gate.shape, BF16),
            pltpu.VMEM(w_up.shape, BF16),
            pltpu.VMEM(w_down.shape, BF16),
            pltpu.VMEM((total_rows, width), BF16),
            *scatter,
            pltpu.VMEM((block, cols), BF16),
            pltpu.VMEM((block, cols), BF16),
            pltpu.VMEM((block, 128), F32),
            pltpu.VMEM((size_d - 1, block, 128), F32),
            pltpu.VMEM((total_rows, cols), BF16),
            pltpu.VMEM((CHUNKS, total_rows, 2 * share), BF16),
            pltpu.VMEM((CHUNKS, slots, local_rows, 2 * share), BF16),
            pltpu.VMEM((CHUNKS, local_rows, 2 * share), BF16),
            pltpu.VMEM((CHUNKS, local_rows, 2 * share), BF16),
            pltpu.VMEM((CHUNKS, total_rows, share), BF16),
            pltpu.VMEM((total_rows, cols), F32),
            *scatter,
            pltpu.SemaphoreType.DMA((4,)),
            pltpu.SemaphoreType.DMA,
            dma_sems(size_d - 1),
            dma_sems(size_d - 1),
            dma_sems((size_s - 1) * size_t),
            dma_sems(size_t - 1),
            dma_sems(size_d - 1),
            dma_sems(size_t - 1),
            dma_sems(size_t * (size_s - 1)),
            dma_sems(CHUNKS * slots),
            dma_sems(CHUNKS),
            dma_sems(CHUNKS * (size_d - 1)),
            dma_sems((size_s - 1) * size_t),
            dma_sems(size_t - 1),
        ],
        compiler_params=pltpu.CompilerParams(
            collective_id=collective_id, has_side_effects=True, vmem_limit_bytes=66000000
        ),
    )(attended, full_rows, gain, w_out, w_gate, w_up, w_down)


def shards(tokens_in, gain_attn, w_query, w_keyval, w_out, gain_mlp, w_gate, w_up, w_down):
    group_index = lax.axis_index(("section", "tensor"))
    data_index = lax.axis_index("dp")
    local_rows = tokens_in.shape[0]
    gathered = ag_group(tokens_in, 1)
    full_rows = jnp.transpose(gathered, (1, 0, 2)).reshape(local_rows, -1)
    normed_attn = rms_scale(full_rows, gain_attn)
    heads_dev = w_query.shape[1] // HD
    group_size = H // KVH
    kv_dev = max(1, heads_dev // group_size)
    positions_local = data_index * local_rows + jnp.arange(local_rows, dtype=jnp.int32)
    keyval_part = jnp.dot(normed_attn, w_keyval, preferred_element_type=jnp.float32).astype(
        jnp.bfloat16
    )
    keyval_rows = jnp.transpose(ag_group(keyval_part, 2), (1, 0, 2)).reshape(local_rows, -1)
    query_proj = jnp.dot(normed_attn, w_query, preferred_element_type=jnp.float32)
    query_rot = rotary(query_proj.reshape(local_rows, heads_dev, HD), positions_local).astype(
        jnp.bfloat16
    )
    first_kv = group_index * heads_dev // group_size
    key_cols = lax.dynamic_slice_in_dim(keyval_rows, first_kv * HD, kv_dev * HD, 1)
    value_cols = lax.dynamic_slice_in_dim(keyval_rows, KVH * HD + first_kv * HD, kv_dev * HD, 1)
    needed = jnp.concatenate([key_cols, value_cols], axis=1)
    kv_all = ag_dp(needed, 3).reshape(-1, needed.shape[1])
    total_rows = kv_all.shape[0]
    key_pos = jnp.arange(total_rows, dtype=jnp.int32)
    key_rot = rotary(
        kv_all[:, : kv_dev * HD].astype(jnp.float32).reshape(total_rows, kv_dev, HD), key_pos
    ).astype(jnp.bfloat16)
    value_all = kv_all[:, kv_dev * HD :].reshape(total_rows, kv_dev, HD)
    query_grp = query_rot.reshape(local_rows, kv_dev, heads_dev // kv_dev, HD)
    scores = jnp.einsum(
        "rkgd,skd->kgrs", query_grp, key_rot, preferred_element_type=jnp.float32
    ) * HD ** (-0.5)
    allowed = key_pos[None, :] <= positions_local[:, None]
    scores = jnp.where(allowed[None, None, :, :], scores, -1e30)
    row_peak = jnp.max(scores, axis=-1, keepdims=True)
    expo_rows = jnp.exp(scores - row_peak)
    prob_rows = (expo_rows / jnp.sum(expo_rows, axis=-1, keepdims=True)).astype(jnp.bfloat16)
    attended = jnp.einsum(
        "kgrs,skd->rkgd", prob_rows, value_all, preferred_element_type=jnp.float32
    )
    attended = attended.astype(jnp.bfloat16).reshape(local_rows, heads_dev * HD)
    cols = w_gate.shape[0]
    gain = lax.dynamic_slice_in_dim(gain_mlp, data_index * cols, cols, 0)[None, :]
    return back(attended, full_rows, gain, w_out, w_gate, w_up, w_down, 4)


def solution(mesh):
    placed = (
        P("dp", ("section", "tensor")),
        P(),
        P(None, ("section", "tensor")),
        P(None, ("section", "tensor")),
        P(("section", "tensor"), None),
        P(),
        P("dp", ("section", "tensor")),
        P("dp", ("section", "tensor")),
        P(("section", "tensor"), "dp"),
    )
    return jax.shard_map(
        shards,
        mesh=mesh,
        in_specs=placed,
        out_specs=P(("section", "tensor"), "dp"),
        check_vma=False,
    )
```

```python
import jax
import jax.numpy as jnp
from jax import lax
from jax.experimental import pallas as pl
from jax.experimental.pallas import tpu as pltpu
from jax.sharding import PartitionSpec as P

H = 64
KVH = 8
HD = 128
EPS = 1e-05
THETA = 10000.0
CHUNKS = 4
MESH = pl.DeviceIdType.MESH
F32 = jnp.float32
BF16 = jnp.bfloat16
VMEM = pl.BlockSpec(memory_space=pltpu.VMEM)
ANY = pl.BlockSpec(memory_space=pl.ANY)


def greet(peers):
    barrier = pltpu.get_barrier_semaphore()
    for peer in peers:
        pl.semaphore_signal(barrier, inc=1, device_id=peer, device_id_type=MESH)
    pl.semaphore_wait(barrier, len(peers))


def push(src, dst, sems, slot, device):
    return pltpu.make_async_remote_copy(
        src_ref=src,
        dst_ref=dst,
        send_sem=sems.at[0, slot],
        recv_sem=sems.at[1, slot],
        device_id=device,
        device_id_type=MESH,
    )


def others(axis):
    size = lax.axis_size(axis)
    me = lax.axis_index(axis)
    return [(step, lax.rem(me + step, size), lax.rem(me + size - step, size)) for step in range(1, size)]


def gather_group(out, at, sem_t, sem_s, on_block=lambda section, tensor, order: None):
    section, tensor = lax.axis_index("section"), lax.axis_index("tensor")
    sections, tensors = others("section"), others("tensor")
    size_t = lax.axis_size("tensor")
    started = []

    def pass_on(block_t, slot):
        for step, to, _ in sections:
            block = out.at[at(section, block_t)]
            copy = push(block, block, sem_s, slot * len(sections) + step - 1, {"section": to})
            copy.start()
            started.append(copy)

    for step, to, _ in tensors:
        block = out.at[at(section, tensor)]
        copy = push(block, block, sem_t, step - 1, {"tensor": to})
        copy.start()
        started.append(copy)
    pass_on(tensor, 0)
    on_block(section, tensor, 0)

    def from_sections(slot):
        for step, to, source in sections:
            source_t = lax.rem(tensor + size_t - slot, size_t)
            block = out.at[at(source, source_t)]
            push(block, block, sem_s, slot * len(sections) + step - 1, {"section": to}).wait_recv()
            on_block(source, source_t, (slot + 1) * len(sections) + slot + step - 1)

    for step, to, source in tensors:
        if step == 1:
            from_sections(0)
        block = out.at[at(section, source)]
        push(block, block, sem_t, step - 1, {"tensor": to}).wait_recv()
        pass_on(source, step)
        on_block(section, source, step * (len(sections) + 1))
        if step > 1:
            from_sections(step - 1)
    from_sections(size_t - 1)
    for copy in started:
        copy.wait_send()


def group_peers():
    return [{"tensor": to} for _, to, _ in others("tensor")] + [
        {"section": to} for _, to, _ in others("section")
    ]


def dma_sems(count):
    return pltpu.SemaphoreType.DMA((2, max(1, count)))


def block_order():
    section, tensor = lax.axis_index("section"), lax.axis_index("tensor")
    size_t = lax.axis_size("tensor")

    def from_sections(slot):
        return [(source, lax.rem(tensor + size_t - slot, size_t)) for _, _, source in others("section")]

    order = [(section, tensor)] + from_sections(0)
    for step, _, source in others("tensor"):
        order.append((section, source))
        if step > 1:
            order += from_sections(step - 1)
    return order + from_sections(size_t - 1)


def front_body(
    x_ref, gain_ref, cos_ref, sin_ref, wq_hbm, wk_hbm, att_ref, full_ref,
    blocks, wq, wk, qacc, kacc, stat, kv_src, kv_dst,
    sem_w, sem_own, sem_t, sem_s, sem_kv, sem_kv_out,
):
    section, tensor, me = lax.axis_index("section"), lax.axis_index("tensor"), lax.axis_index("dp")
    size_s, size_t, size_d = lax.axis_size("section"), lax.axis_size("tensor"), lax.axis_size("dp")
    count = size_s * size_t
    index = section * size_t + tensor
    local_rows, width = x_ref.shape
    features = count * width
    heads_dev = qacc.shape[1] // HD
    group_size = H // KVH
    units, _, unit = kv_src.shape
    pieces = HD // unit
    rep = group_size // heads_dev

    order = block_order()
    loads = []
    for k, (s, t) in enumerate(order):
        rows = pl.ds(pl.multiple_of((s * size_t + t) * width, width), width)
        loads.append(
            (
                pltpu.make_async_copy(wq_hbm.at[rows], wq.at[k], sem_w.at[0, k]),
                pltpu.make_async_copy(wk_hbm.at[rows], wk.at[k], sem_w.at[1, k]),
            )
        )
    for pair in loads:
        for load in pair:
            load.start()
    own = pltpu.make_async_copy(x_ref, blocks.at[index], sem_own)
    own.start()

    dps = others("dp")
    everyone = []
    for hop_s in range(size_s):
        for hop_t in range(size_t):
            for hop_d in range(size_d):
                if hop_s + hop_t + hop_d:
                    everyone.append(
                        {
                            "section": lax.rem(section + hop_s, size_s),
                            "tensor": lax.rem(tensor + hop_t, size_t),
                            "dp": lax.rem(me + hop_d, size_d),
                        }
                    )
    greet(everyone)
    own.wait()

    seen = []

    def on_block(s, t, _):
        k = len(seen)
        seen.append(k)
        for load in loads[k]:
            load.wait()
        at = s * size_t + t
        raw = blocks[at]
        full_ref[:, pl.ds(pl.multiple_of(at * width, width), width)] = raw
        rows = raw.astype(F32)
        part = jnp.sum(rows * rows, axis=-1, keepdims=True)
        stat[...] = part if k == 0 else stat[...] + part
        scaled = (rows * gain_ref[at].astype(F32)).astype(BF16)
        tile = tile_of(qacc.shape[1], 256)

        @pl.loop(0, qacc.shape[1] // tile)
        def _(j):
            cols = pl.ds(pl.multiple_of(j * tile, tile), tile)
            term = jnp.dot(scaled, wq[k, :, cols], preferred_element_type=F32)
            qacc[:, cols] = term if k == 0 else qacc[:, cols] + term

        term = jnp.dot(scaled, wk[k], preferred_element_type=F32)
        kacc[...] = term if k == 0 else kacc[...] + term

    gather_group(blocks, lambda s, t: s * size_t + t, sem_t, sem_s, on_block)
    factor = lax.rsqrt(stat[...] * (1.0 / features) + EPS)

    for i in range(units):
        kv_src[i] = (kacc[:, i * unit : (i + 1) * unit] * factor).astype(BF16)

    def dp_rows(at):
        return pl.ds(pl.multiple_of(at * local_rows, local_rows), local_rows)

    half = KVH * pieces

    def kv_copy(i, r, g, kind, piece, step, to):
        return pltpu.make_async_remote_copy(
            src_ref=kv_src.at[i],
            dst_ref=kv_dst.at[kind, piece, dp_rows(me)],
            send_sem=sem_kv_out.at[(i * rep + r) * size_d + step],
            recv_sem=sem_kv.at[1, (kind * pieces + piece) * size_d + step],
            device_id={"section": g // size_t, "tensor": lax.rem(g, size_t), "dp": to},
            device_id_type=MESH,
        )

    hops = [(step, to, source) for step, to, source in dps] + [(0, me, me)]

    def each_send(act):
        for i in range(units):
            u = index * units + i
            kind, piece = u // half, lax.rem(u, pieces)
            head = lax.rem(u, half) // pieces
            for r in range(rep):
                g = head * rep + r
                for step, to, _ in hops:
                    if step:
                        act(kv_copy(i, r, g, kind, piece, step, to), i, kind, piece, False)
                    else:
                        @pl.when(g != index)
                        def _():
                            act(kv_copy(i, r, g, kind, piece, step, to), i, kind, piece, False)

                        @pl.when(g == index)
                        def _():
                            act(None, i, kind, piece, True)

    def begin(copy, i, kind, piece, local):
        if local:
            kv_dst[kind, piece, dp_rows(me), :] = kv_src[i]
        else:
            copy.start()

    each_send(begin)

    cosine, sine = cos_ref[dp_rows(me), :], sin_ref[dp_rows(me), :]
    queries = []
    for h in range(heads_dev):
        q = qacc[:, h * HD : (h + 1) * HD] * factor
        q = q * cosine + pltpu.roll(q, HD // 2, axis=1) * sine
        queries.append(q.astype(BF16))

    head = index // rep
    for kind in range(2):
        for piece in range(pieces):
            g = (kind * half + head * pieces + piece) // units
            for step, to, source in hops:
                dst = kv_dst.at[kind, piece, dp_rows(source)]
                wait = push(dst, dst, sem_kv, (kind * pieces + piece) * size_d + step, {"tensor": tensor})
                if step:
                    wait.wait_recv()
                else:
                    @pl.when(g != index)
                    def _():
                        wait.wait_recv()

    def whole(kind):
        return jnp.concatenate([kv_dst[kind, piece] for piece in range(pieces)], axis=1) if pieces > 1 else kv_dst[kind, 0]

    keys = whole(0).astype(F32)
    keys = (keys * cos_ref[...] + pltpu.roll(keys, HD // 2, axis=1) * sin_ref[...]).astype(BF16)
    values = whole(1)
    total_rows = keys.shape[0]
    shape = (local_rows, total_rows)
    allowed = lax.broadcasted_iota(jnp.int32, shape, 1) <= (
        lax.broadcasted_iota(jnp.int32, shape, 0) + me * local_rows
    )
    for h in range(heads_dev):
        scores = lax.dot_general(
            queries[h], keys, (((1,), (1,)), ((), ())), preferred_element_type=F32
        ) * HD ** (-0.5)
        scores = jnp.where(allowed, scores, -1e30)
        expo = jnp.exp(scores - jnp.max(scores, axis=-1, keepdims=True))
        probs = (expo / jnp.sum(expo, axis=-1, keepdims=True)).astype(BF16)
        att_ref[:, h * HD : (h + 1) * HD] = jnp.dot(
            probs, values, preferred_element_type=F32
        ).astype(BF16)

    def end(copy, i, kind, piece, local):
        if not local:
            copy.wait_send()

    each_send(end)


def front(tokens, gain, cosine, sine, w_query, w_keyval, collective_id):
    size_s, size_t, size_d = lax.axis_size("section"), lax.axis_size("tensor"), lax.axis_size("dp")
    count = size_s * size_t
    local_rows, width = tokens.shape
    kv_cols = w_keyval.shape[1]
    unit = min(kv_cols, HD)
    pieces = HD // unit
    rep = (H // KVH) // (w_query.shape[1] // HD)
    arrivals = 2 * pieces * size_d
    return pl.pallas_call(
        front_body,
        out_shape=(
            jax.ShapeDtypeStruct((local_rows, w_query.shape[1]), BF16),
            jax.ShapeDtypeStruct((local_rows, count * width), BF16),
        ),
        in_specs=[VMEM, VMEM, VMEM, VMEM, ANY, ANY],
        out_specs=(VMEM, VMEM),
        scratch_shapes=[
            pltpu.VMEM((count, local_rows, width), BF16),
            pltpu.VMEM((count, width, w_query.shape[1]), BF16),
            pltpu.VMEM((count, width, kv_cols), BF16),
            pltpu.VMEM((local_rows, w_query.shape[1]), F32),
            pltpu.VMEM((local_rows, kv_cols), F32),
            pltpu.VMEM((local_rows, 1), F32),
            pltpu.VMEM((kv_cols // unit, local_rows, unit), BF16),
            pltpu.VMEM((2, pieces, local_rows * size_d, unit), BF16),
            pltpu.SemaphoreType.DMA((2, count)),
            pltpu.SemaphoreType.DMA,
            dma_sems(size_t - 1),
            dma_sems(size_t * (size_s - 1)),
            dma_sems(arrivals),
            pltpu.SemaphoreType.DMA((kv_cols // unit * rep * size_d,)),
        ],
        compiler_params=pltpu.CompilerParams(
            collective_id=collective_id, has_side_effects=True, vmem_limit_bytes=66000000
        ),
    )(tokens, gain, cosine, sine, w_query, w_keyval)


def tile_of(width, most):
    return width if width <= most else most


def scatter_group(part, pair_rx, comb, z_rx, sem_p, sem_z):
    section, tensor = lax.axis_index("section"), lax.axis_index("tensor")
    size_t = lax.axis_size("tensor")
    block = z_rx.shape[1]

    def rows(s, t):
        return pl.ds(pl.multiple_of((s * size_t + t) * block, block), block)

    sections, tensors = others("section"), others("tensor")
    order = [(step, to) for step, to, _ in tensors] + [(0, tensor)]
    started = []
    for step, to in order:
        for hop, other, _ in sections:
            copy = push(
                part.at[rows(other, to)],
                pair_rx.at[hop - 1, step],
                sem_p,
                (hop - 1) * size_t + step,
                {"section": other},
            )
            copy.start()
            started.append(copy)

    def paired(step, to):
        total = part[rows(section, to), :].astype(F32)
        for hop, other, _ in sections:
            push(
                part.at[rows(other, to)],
                pair_rx.at[hop - 1, step],
                sem_p,
                (hop - 1) * size_t + step,
                {"section": other},
            ).wait_recv()
            total = total + pair_rx[hop - 1, step].astype(F32)
        return total

    for step, to, _ in tensors:
        comb[step - 1] = paired(step, to).astype(BF16)
        copy = push(comb.at[step - 1], z_rx.at[step - 1], sem_z, step - 1, {"tensor": to})
        copy.start()
        started.append(copy)
    total = paired(0, tensor)
    for step, to, _ in tensors:
        push(comb.at[step - 1], z_rx.at[step - 1], sem_z, step - 1, {"tensor": to}).wait_recv()
        total = total + z_rx[step - 1].astype(F32)
    for copy in started:
        copy.wait_send()
    return total


def back_body(
    att_ref, rows_ref, gain_ref, wo_hbm, wg_hbm, wu_hbm, wd_hbm, out_ref,
    wo, wg, wu, wd, att_all, part, pair_rx, comb, z_rx, resid, mid, stat_tx, stat_rx,
    nrm, gu, rx1, tx2, rx2, hid, acc, part2, pair_rx2, comb2, z_rx2,
    sem_w, sem_own, sem_att, sem_res, sem_p, sem_z, sem_stat, sem_t, sem_s,
    sem_1, sem_2, sem_h, sem_p2, sem_z2,
):
    section, tensor, me = lax.axis_index("section"), lax.axis_index("tensor"), lax.axis_index("dp")
    size_t, size_d = lax.axis_size("tensor"), lax.axis_size("dp")
    group_index = section * size_t + tensor
    local_rows, width = att_ref.shape
    block, cols = mid.shape
    total_rows = att_all.shape[0]
    features = rows_ref.shape[1]
    dps = others("dp")
    sends = []

    loads = [
        pltpu.make_async_copy(wo_hbm.at[:, pl.ds(pl.multiple_of(me * cols, cols), cols)], wo, sem_w.at[0]),
        pltpu.make_async_copy(wg_hbm, wg, sem_w.at[1]),
        pltpu.make_async_copy(wu_hbm, wu, sem_w.at[2]),
        pltpu.make_async_copy(wd_hbm, wd, sem_w.at[3]),
    ]
    for load in loads:
        load.start()

    greet(group_peers() + [{"dp": to} for _, to, _ in dps])

    def dp_rows(index):
        return pl.ds(pl.multiple_of(index * local_rows, local_rows), local_rows)

    for step, to, _ in dps:
        copy = push(att_ref, att_all.at[dp_rows(me)], sem_att, step - 1, {"dp": to})
        copy.start()
        sends.append(copy)

    per = local_rows // block
    holder = group_index // per
    held_rows = pl.ds(pl.multiple_of(lax.rem(group_index, per) * block, block), block)

    def resid_copy(step, to):
        src = rows_ref.at[held_rows, pl.ds(pl.multiple_of(to * cols, cols), cols)]
        return push(src, resid, sem_res, step - 1, {"dp": to})

    @pl.when(me == holder)
    def _():
        for step, to, _ in dps:
            resid_copy(step, to).start()
        resid[...] = rows_ref[held_rows, pl.ds(pl.multiple_of(me * cols, cols), cols)]

    att_all[dp_rows(me), :] = att_ref[...]
    loads[0].wait()
    tile = tile_of(cols, 512)

    def out_part(index):
        lines = att_all[dp_rows(index), :]

        @pl.loop(0, cols // tile)
        def _(j):
            at = pl.ds(pl.multiple_of(j * tile, tile), tile)
            part[dp_rows(index), at] = jnp.dot(lines, wo[:, at], preferred_element_type=F32).astype(BF16)

    out_part(me)
    for step, to, source in dps:
        push(att_ref, att_all.at[dp_rows(source)], sem_att, step - 1, {"dp": to}).wait_recv()
        out_part(source)

    summed = scatter_group(part, pair_rx, comb, z_rx, sem_p, sem_z)

    for step, to, source in dps:
        @pl.when(source == holder)
        def _():
            resid_copy(step, to).wait_recv()

    @pl.when(me == holder)
    def _():
        for step, to, _ in dps:
            resid_copy(step, to).wait_send()

    mid_rows = (resid[...].astype(F32) + summed).astype(BF16)
    mid[...] = mid_rows
    squares = mid_rows.astype(F32)
    stat = jnp.sum(squares * squares, axis=-1, keepdims=True)
    stat_tx[...] = jnp.broadcast_to(stat, stat_tx.shape)
    for step, to, _ in dps:
        copy = push(stat_tx, stat_rx.at[step - 1], sem_stat, step - 1, {"dp": to})
        copy.start()
        sends.append(copy)
    for step, to, _ in dps:
        push(stat_tx, stat_rx.at[step - 1], sem_stat, step - 1, {"dp": to}).wait_recv()
        stat = stat + stat_rx[step - 1][:, :1]
    factor = lax.rsqrt(stat * (1.0 / features) + EPS)

    def token_rows(s, t):
        return pl.ds(pl.multiple_of((s * size_t + t) * block, block), block)

    nrm[token_rows(section, tensor), :] = (
        mid[...].astype(F32) * factor * gain_ref[...].astype(F32)
    ).astype(BF16)
    gather_group(nrm, token_rows, sem_t, sem_s)

    loads[1].wait()
    loads[2].wait()
    share = gu.shape[2] // 2
    gtile = tile_of(share, 256)
    square = size_d == 4
    if square:
        x, y = lax.rem(me, 2), me // 2
        near = [y * 2 + (1 - x), (1 - y) * 2 + x]
        far = (1 - y) * 2 + (1 - x)
    for c in range(CHUNKS):
        @pl.loop(0, share // gtile)
        def _(j):
            src = pl.ds(pl.multiple_of(c * share + j * gtile, gtile), gtile)
            lo = pl.ds(pl.multiple_of(j * gtile, gtile), gtile)
            hi = pl.ds(pl.multiple_of(share + j * gtile, gtile), gtile)
            gu[c, :, lo] = jnp.dot(nrm[...], wg[:, src], preferred_element_type=F32).astype(BF16)
            gu[c, :, hi] = jnp.dot(nrm[...], wu[:, src], preferred_element_type=F32).astype(BF16)

        if square:
            first = near[c % 2]
            for slot, owner in ((1, far), (0, first)):
                copy = push(gu.at[c, dp_rows(owner)], rx1.at[c, slot], sem_1, 2 * c + slot, {"dp": first})
                copy.start()
                sends.append(copy)
        else:
            for step, to, _ in dps:
                slot = step - 1
                copy = push(gu.at[c, dp_rows(to)], rx1.at[c, slot], sem_1, (size_d - 1) * c + slot, {"dp": to})
                copy.start()
                sends.append(copy)

    if square:
        for c in range(CHUNKS):
            first, second = near[c % 2], near[1 - c % 2]
            push(gu.at[c, dp_rows(far)], rx1.at[c, 1], sem_1, 2 * c + 1, {"dp": first}).wait_recv()
            tx2[c] = (gu[c, dp_rows(second), :].astype(F32) + rx1[c, 1].astype(F32)).astype(BF16)
            copy = push(tx2.at[c], rx2.at[c], sem_2, c, {"dp": second})
            copy.start()
            sends.append(copy)

    hid_slots = size_d - 1
    for c in range(CHUNKS):
        both = gu[c, dp_rows(me), :].astype(F32)
        if square:
            first, second = near[c % 2], near[1 - c % 2]
            push(gu.at[c, dp_rows(first)], rx1.at[c, 0], sem_1, 2 * c, {"dp": first}).wait_recv()
            push(tx2.at[c], rx2.at[c], sem_2, c, {"dp": second}).wait_recv()
            both = both + rx1[c, 0].astype(F32) + rx2[c].astype(F32)
        else:
            for step, to, _ in dps:
                slot = step - 1
                push(
                    gu.at[c, dp_rows(to)], rx1.at[c, slot], sem_1, (size_d - 1) * c + slot, {"dp": to}
                ).wait_recv()
                both = both + rx1[c, slot].astype(F32)
        gate, up = both[:, :share], both[:, share:]
        hid[c, dp_rows(me), :] = (gate / (1.0 + jnp.exp(-gate)) * up).astype(BF16)
        mine = hid.at[c, dp_rows(me)]
        targets = list(enumerate(near)) if square else [(step - 1, to) for step, to, _ in dps]
        for slot, to in targets:
            copy = push(mine, mine, sem_h, hid_slots * c + slot, {"dp": to})
            copy.start()
            sends.append(copy)

    if square:
        for c in range(CHUNKS):
            one, two = c % 2, 1 - c % 2
            theirs = hid.at[c, dp_rows(near[one])]
            push(theirs, theirs, sem_h, hid_slots * c + one, {"dp": near[one]}).wait_recv()
            copy = push(theirs, theirs, sem_h, hid_slots * c + 2, {"dp": near[two]})
            copy.start()
            sends.append(copy)

    loads[3].wait()
    for c in range(CHUNKS):
        if square:
            two = 1 - c % 2
            arrivals = [(two, near[two]), (2, far)]
        else:
            arrivals = [(step - 1, source) for step, _, source in dps]
        for slot, source in arrivals:
            theirs = hid.at[c, dp_rows(source)]
            push(theirs, theirs, sem_h, hid_slots * c + slot, {"dp": source}).wait_recv()

        @pl.loop(0, cols // tile)
        def _(j):
            at = pl.ds(pl.multiple_of(j * tile, tile), tile)
            term = jnp.dot(hid[c], wd[c * share : (c + 1) * share, at], preferred_element_type=F32)
            if c > 0:
                term = acc[:, at] + term
            if c < CHUNKS - 1:
                acc[:, at] = term
            else:
                part2[:, at] = term.astype(BF16)

    total = scatter_group(part2, pair_rx2, comb2, z_rx2, sem_p2, sem_z2)
    out_ref[...] = (mid[...].astype(F32) + total).astype(BF16)
    for copy in sends:
        copy.wait_send()


def back(attended, full_rows, gain, w_out, w_gate, w_up, w_down, collective_id):
    size_s, size_t, size_d = lax.axis_size("section"), lax.axis_size("tensor"), lax.axis_size("dp")
    local_rows, width = attended.shape
    total_rows = local_rows * size_d
    block = total_rows // (size_s * size_t)
    cols, hidden = w_gate.shape
    share = hidden // CHUNKS
    slots = 2 if size_d == 4 else size_d - 1
    scatter = [
        pltpu.VMEM((total_rows, cols), BF16),
        pltpu.VMEM((size_s - 1, size_t, block, cols), BF16),
        pltpu.VMEM((size_t - 1, block, cols), BF16),
        pltpu.VMEM((size_t - 1, block, cols), BF16),
    ]
    return pl.pallas_call(
        back_body,
        out_shape=jax.ShapeDtypeStruct((block, cols), BF16),
        in_specs=[VMEM, VMEM, VMEM, ANY, ANY, ANY, ANY],
        out_specs=VMEM,
        scratch_shapes=[
            pltpu.VMEM((width, cols), BF16),
            pltpu.VMEM(w_gate.shape, BF16),
            pltpu.VMEM(w_up.shape, BF16),
            pltpu.VMEM(w_down.shape, BF16),
            pltpu.VMEM((total_rows, width), BF16),
            *scatter,
            pltpu.VMEM((block, cols), BF16),
            pltpu.VMEM((block, cols), BF16),
            pltpu.VMEM((block, 128), F32),
            pltpu.VMEM((size_d - 1, block, 128), F32),
            pltpu.VMEM((total_rows, cols), BF16),
            pltpu.VMEM((CHUNKS, total_rows, 2 * share), BF16),
            pltpu.VMEM((CHUNKS, slots, local_rows, 2 * share), BF16),
            pltpu.VMEM((CHUNKS, local_rows, 2 * share), BF16),
            pltpu.VMEM((CHUNKS, local_rows, 2 * share), BF16),
            pltpu.VMEM((CHUNKS, total_rows, share), BF16),
            pltpu.VMEM((total_rows, cols), F32),
            *scatter,
            pltpu.SemaphoreType.DMA((4,)),
            pltpu.SemaphoreType.DMA,
            dma_sems(size_d - 1),
            dma_sems(size_d - 1),
            dma_sems((size_s - 1) * size_t),
            dma_sems(size_t - 1),
            dma_sems(size_d - 1),
            dma_sems(size_t - 1),
            dma_sems(size_t * (size_s - 1)),
            dma_sems(CHUNKS * slots),
            dma_sems(CHUNKS),
            dma_sems(CHUNKS * (size_d - 1)),
            dma_sems((size_s - 1) * size_t),
            dma_sems(size_t - 1),
        ],
        compiler_params=pltpu.CompilerParams(
            collective_id=collective_id, has_side_effects=True, vmem_limit_bytes=66000000
        ),
    )(attended, full_rows, gain, w_out, w_gate, w_up, w_down)


def shards(tokens_in, gain_attn, w_query, w_keyval, w_out, gain_mlp, w_gate, w_up, w_down):
    data_index = lax.axis_index("dp")
    local_rows, width = tokens_in.shape
    total_rows = local_rows * lax.axis_size("dp")
    half_dim = HD // 2
    frequency = THETA ** (-jnp.arange(half_dim, dtype=jnp.float32) * 2.0 / HD)
    angles = jnp.arange(total_rows, dtype=jnp.int32).astype(F32)[:, None] * frequency[None, :]
    cosine, sine = jnp.cos(angles), jnp.sin(angles)
    attended, full_rows = front(
        tokens_in,
        gain_attn.reshape(-1, 1, width),
        jnp.concatenate([cosine, cosine], axis=1),
        jnp.concatenate([-sine, sine], axis=1),
        w_query,
        w_keyval,
        1,
    )
    cols = w_gate.shape[0]
    gain = lax.dynamic_slice_in_dim(gain_mlp, data_index * cols, cols, 0)[None, :]
    return back(attended, full_rows, gain, w_out, w_gate, w_up, w_down, 2)


def solution(mesh):
    placed = (
        P("dp", ("section", "tensor")),
        P(),
        P(None, ("section", "tensor")),
        P(None, ("section", "tensor")),
        P(("section", "tensor"), None),
        P(),
        P("dp", ("section", "tensor")),
        P("dp", ("section", "tensor")),
        P(("section", "tensor"), "dp"),
    )
    return jax.shard_map(
        shards,
        mesh=mesh,
        in_specs=placed,
        out_specs=P(("section", "tensor"), "dp"),
        check_vma=False,
    )
```

```python
import jax
import jax.numpy as jnp
from jax import lax
from jax.experimental import pallas as pl
from jax.experimental.pallas import tpu as pltpu
from jax.sharding import PartitionSpec as P

H = 64
KVH = 8
HD = 128
EPS = 1e-05
THETA = 10000.0
CHUNKS = 8
MESH = pl.DeviceIdType.MESH
F32 = jnp.float32
BF16 = jnp.bfloat16
VMEM = pl.BlockSpec(memory_space=pltpu.VMEM)
ANY = pl.BlockSpec(memory_space=pl.ANY)


def greet(peers):
    barrier = pltpu.get_barrier_semaphore()
    for peer in peers:
        pl.semaphore_signal(barrier, inc=1, device_id=peer, device_id_type=MESH)
    pl.semaphore_wait(barrier, len(peers))


def push(src, dst, sems, slot, device):
    return pltpu.make_async_remote_copy(
        src_ref=src,
        dst_ref=dst,
        send_sem=sems.at[0, slot],
        recv_sem=sems.at[1, slot],
        device_id=device,
        device_id_type=MESH,
    )


def others(axis):
    size = lax.axis_size(axis)
    me = lax.axis_index(axis)
    return [(step, lax.rem(me + step, size), lax.rem(me + size - step, size)) for step in range(1, size)]


def gather_group(out, at, sem_t, sem_s, on_block=lambda section, tensor, order: None):
    section, tensor = lax.axis_index("section"), lax.axis_index("tensor")
    sections, tensors = others("section"), others("tensor")
    size_t = lax.axis_size("tensor")
    started = []

    def pass_on(block_t, slot):
        for step, to, _ in sections:
            block = out.at[at(section, block_t)]
            copy = push(block, block, sem_s, slot * len(sections) + step - 1, {"section": to})
            copy.start()
            started.append(copy)

    for step, to, _ in tensors:
        block = out.at[at(section, tensor)]
        copy = push(block, block, sem_t, step - 1, {"tensor": to})
        copy.start()
        started.append(copy)
    pass_on(tensor, 0)
    on_block(section, tensor, 0)

    def from_sections(slot):
        for step, to, source in sections:
            source_t = lax.rem(tensor + size_t - slot, size_t)
            block = out.at[at(source, source_t)]
            push(block, block, sem_s, slot * len(sections) + step - 1, {"section": to}).wait_recv()
            on_block(source, source_t, (slot + 1) * len(sections) + slot + step - 1)

    for step, to, source in tensors:
        if step == 1:
            from_sections(0)
        block = out.at[at(section, source)]
        push(block, block, sem_t, step - 1, {"tensor": to}).wait_recv()
        pass_on(source, step)
        on_block(section, source, step * (len(sections) + 1))
        if step > 1:
            from_sections(step - 1)
    from_sections(size_t - 1)
    for copy in started:
        copy.wait_send()


def group_peers():
    return [{"tensor": to} for _, to, _ in others("tensor")] + [
        {"section": to} for _, to, _ in others("section")
    ]


def dma_sems(count):
    return pltpu.SemaphoreType.DMA((2, max(1, count)))


def block_order():
    section, tensor = lax.axis_index("section"), lax.axis_index("tensor")
    size_t = lax.axis_size("tensor")

    def from_sections(slot):
        return [(source, lax.rem(tensor + size_t - slot, size_t)) for _, _, source in others("section")]

    order = [(section, tensor)] + from_sections(0)
    for step, _, source in others("tensor"):
        order.append((section, source))
        if step > 1:
            order += from_sections(step - 1)
    return order + from_sections(size_t - 1)


def front_body(
    x_ref, gain_ref, cos_ref, sin_ref, wq_hbm, wk_hbm, att_ref, full_ref,
    blocks, wq, wk, qacc, kacc, stat, kv_src, kv_dst,
    sem_w, sem_own, sem_t, sem_s, sem_kv, sem_kv_out,
):
    section, tensor, me = lax.axis_index("section"), lax.axis_index("tensor"), lax.axis_index("dp")
    size_s, size_t, size_d = lax.axis_size("section"), lax.axis_size("tensor"), lax.axis_size("dp")
    count = size_s * size_t
    index = section * size_t + tensor
    local_rows, width = x_ref.shape
    features = count * width
    heads_dev = qacc.shape[1] // HD
    group_size = H // KVH
    units, _, unit = kv_src.shape
    pieces = HD // unit
    rep = group_size // heads_dev

    order = block_order()
    loads = []
    for k, (s, t) in enumerate(order):
        rows = pl.ds(pl.multiple_of((s * size_t + t) * width, width), width)
        loads.append(
            (
                pltpu.make_async_copy(wq_hbm.at[rows], wq.at[k], sem_w.at[0, k]),
                pltpu.make_async_copy(wk_hbm.at[rows], wk.at[k], sem_w.at[1, k]),
            )
        )
    for pair in loads:
        for load in pair:
            load.start()
    own = pltpu.make_async_copy(x_ref, blocks.at[index], sem_own)
    own.start()

    dps = others("dp")
    everyone = []
    for hop_s in range(size_s):
        for hop_t in range(size_t):
            for hop_d in range(size_d):
                if hop_s + hop_t + hop_d:
                    everyone.append(
                        {
                            "section": lax.rem(section + hop_s, size_s),
                            "tensor": lax.rem(tensor + hop_t, size_t),
                            "dp": lax.rem(me + hop_d, size_d),
                        }
                    )
    greet(everyone)
    own.wait()

    seen = []

    def on_block(s, t, _):
        k = len(seen)
        seen.append(k)
        for load in loads[k]:
            load.wait()
        at = s * size_t + t
        raw = blocks[at]
        full_ref[:, pl.ds(pl.multiple_of(at * width, width), width)] = raw
        rows = raw.astype(F32)
        part = jnp.sum(rows * rows, axis=-1, keepdims=True)
        stat[...] = part if k == 0 else stat[...] + part
        scaled = (rows * gain_ref[at].astype(F32)).astype(BF16)
        tile = tile_of(qacc.shape[1], 256)

        @pl.loop(0, qacc.shape[1] // tile)
        def _(j):
            cols = pl.ds(pl.multiple_of(j * tile, tile), tile)
            term = jnp.dot(scaled, wq[k, :, cols], preferred_element_type=F32)
            qacc[:, cols] = term if k == 0 else qacc[:, cols] + term

        term = jnp.dot(scaled, wk[k], preferred_element_type=F32)
        kacc[...] = term if k == 0 else kacc[...] + term

    gather_group(blocks, lambda s, t: s * size_t + t, sem_t, sem_s, on_block)
    factor = lax.rsqrt(stat[...] * (1.0 / features) + EPS)

    for i in range(units):
        kv_src[i] = (kacc[:, i * unit : (i + 1) * unit] * factor).astype(BF16)

    def dp_rows(at):
        return pl.ds(pl.multiple_of(at * local_rows, local_rows), local_rows)

    half = KVH * pieces

    def kv_copy(i, r, g, kind, piece, step, to):
        return pltpu.make_async_remote_copy(
            src_ref=kv_src.at[i],
            dst_ref=kv_dst.at[kind, piece, dp_rows(me)],
            send_sem=sem_kv_out.at[(i * rep + r) * size_d + step],
            recv_sem=sem_kv.at[1, (kind * pieces + piece) * size_d + step],
            device_id={"section": g // size_t, "tensor": lax.rem(g, size_t), "dp": to},
            device_id_type=MESH,
        )

    hops = [(step, to, source) for step, to, source in dps] + [(0, me, me)]

    def each_send(act):
        for i in range(units):
            u = index * units + i
            kind, piece = u // half, lax.rem(u, pieces)
            head = lax.rem(u, half) // pieces
            for r in range(rep):
                g = head * rep + r
                for step, to, _ in hops:
                    if step:
                        act(kv_copy(i, r, g, kind, piece, step, to), i, kind, piece, False)
                    else:
                        @pl.when(g != index)
                        def _():
                            act(kv_copy(i, r, g, kind, piece, step, to), i, kind, piece, False)

                        @pl.when(g == index)
                        def _():
                            act(None, i, kind, piece, True)

    def begin(copy, i, kind, piece, local):
        if local:
            kv_dst[kind, piece, dp_rows(me), :] = kv_src[i]
        else:
            copy.start()

    each_send(begin)

    cosine, sine = cos_ref[dp_rows(me), :], sin_ref[dp_rows(me), :]
    queries = []
    for h in range(heads_dev):
        q = qacc[:, h * HD : (h + 1) * HD] * factor
        q = q * cosine + pltpu.roll(q, HD // 2, axis=1) * sine
        queries.append(q.astype(BF16))

    head = index // rep
    for kind in range(2):
        for piece in range(pieces):
            g = (kind * half + head * pieces + piece) // units
            for step, to, source in hops:
                dst = kv_dst.at[kind, piece, dp_rows(source)]
                wait = push(dst, dst, sem_kv, (kind * pieces + piece) * size_d + step, {"tensor": tensor})
                if step:
                    wait.wait_recv()
                else:
                    @pl.when(g != index)
                    def _():
                        wait.wait_recv()

    def whole(kind):
        return jnp.concatenate([kv_dst[kind, piece] for piece in range(pieces)], axis=1) if pieces > 1 else kv_dst[kind, 0]

    keys = whole(0).astype(F32)
    keys = (keys * cos_ref[...] + pltpu.roll(keys, HD // 2, axis=1) * sin_ref[...]).astype(BF16)
    values = whole(1)
    total_rows = keys.shape[0]
    shape = (local_rows, total_rows)
    allowed = lax.broadcasted_iota(jnp.int32, shape, 1) <= (
        lax.broadcasted_iota(jnp.int32, shape, 0) + me * local_rows
    )
    for h in range(heads_dev):
        scores = lax.dot_general(
            queries[h], keys, (((1,), (1,)), ((), ())), preferred_element_type=F32
        ) * HD ** (-0.5)
        scores = jnp.where(allowed, scores, -1e30)
        expo = jnp.exp(scores - jnp.max(scores, axis=-1, keepdims=True))
        probs = (expo / jnp.sum(expo, axis=-1, keepdims=True)).astype(BF16)
        att_ref[:, h * HD : (h + 1) * HD] = jnp.dot(
            probs, values, preferred_element_type=F32
        ).astype(BF16)

    def end(copy, i, kind, piece, local):
        if not local:
            copy.wait_send()

    each_send(end)


def front(tokens, gain, cosine, sine, w_query, w_keyval, collective_id):
    size_s, size_t, size_d = lax.axis_size("section"), lax.axis_size("tensor"), lax.axis_size("dp")
    count = size_s * size_t
    local_rows, width = tokens.shape
    kv_cols = w_keyval.shape[1]
    unit = min(kv_cols, HD)
    pieces = HD // unit
    rep = (H // KVH) // (w_query.shape[1] // HD)
    arrivals = 2 * pieces * size_d
    return pl.pallas_call(
        front_body,
        out_shape=(
            jax.ShapeDtypeStruct((local_rows, w_query.shape[1]), BF16),
            jax.ShapeDtypeStruct((local_rows, count * width), BF16),
        ),
        in_specs=[VMEM, VMEM, VMEM, VMEM, ANY, ANY],
        out_specs=(VMEM, VMEM),
        scratch_shapes=[
            pltpu.VMEM((count, local_rows, width), BF16),
            pltpu.VMEM((count, width, w_query.shape[1]), BF16),
            pltpu.VMEM((count, width, kv_cols), BF16),
            pltpu.VMEM((local_rows, w_query.shape[1]), F32),
            pltpu.VMEM((local_rows, kv_cols), F32),
            pltpu.VMEM((local_rows, 1), F32),
            pltpu.VMEM((kv_cols // unit, local_rows, unit), BF16),
            pltpu.VMEM((2, pieces, local_rows * size_d, unit), BF16),
            pltpu.SemaphoreType.DMA((2, count)),
            pltpu.SemaphoreType.DMA,
            dma_sems(size_t - 1),
            dma_sems(size_t * (size_s - 1)),
            dma_sems(arrivals),
            pltpu.SemaphoreType.DMA((kv_cols // unit * rep * size_d,)),
        ],
        compiler_params=pltpu.CompilerParams(
            collective_id=collective_id, has_side_effects=True, vmem_limit_bytes=66000000
        ),
    )(tokens, gain, cosine, sine, w_query, w_keyval)


def tile_of(width, most):
    return width if width <= most else most


def scatter_group(part, pair_rx, comb, z_rx, sem_p, sem_z):
    section, tensor = lax.axis_index("section"), lax.axis_index("tensor")
    size_t = lax.axis_size("tensor")
    block = z_rx.shape[1]

    def rows(s, t):
        return pl.ds(pl.multiple_of((s * size_t + t) * block, block), block)

    sections, tensors = others("section"), others("tensor")
    order = [(step, to) for step, to, _ in tensors] + [(0, tensor)]
    started = []
    for step, to in order:
        for hop, other, _ in sections:
            copy = push(
                part.at[rows(other, to)],
                pair_rx.at[hop - 1, step],
                sem_p,
                (hop - 1) * size_t + step,
                {"section": other},
            )
            copy.start()
            started.append(copy)

    def paired(step, to):
        total = part[rows(section, to), :].astype(F32)
        for hop, other, _ in sections:
            push(
                part.at[rows(other, to)],
                pair_rx.at[hop - 1, step],
                sem_p,
                (hop - 1) * size_t + step,
                {"section": other},
            ).wait_recv()
            total = total + pair_rx[hop - 1, step].astype(F32)
        return total

    for step, to, _ in tensors:
        comb[step - 1] = paired(step, to).astype(BF16)
        copy = push(comb.at[step - 1], z_rx.at[step - 1], sem_z, step - 1, {"tensor": to})
        copy.start()
        started.append(copy)
    total = paired(0, tensor)
    for step, to, _ in tensors:
        push(comb.at[step - 1], z_rx.at[step - 1], sem_z, step - 1, {"tensor": to}).wait_recv()
        total = total + z_rx[step - 1].astype(F32)
    for copy in started:
        copy.wait_send()
    return total


def back_body(
    att_ref, rows_ref, gain_ref, wo_hbm, wg_hbm, wu_hbm, wd_hbm, out_ref,
    wo, wg, wu, wd, att_all, part, pair_rx, comb, z_rx, resid, mid, stat_tx, stat_rx,
    nrm, gu, rx1, tx2, rx2, hid, acc, part2, pair_rx2, comb2, z_rx2,
    sem_w, sem_own, sem_att, sem_res, sem_p, sem_z, sem_stat, sem_t, sem_s,
    sem_1, sem_2, sem_h, sem_p2, sem_z2,
):
    section, tensor, me = lax.axis_index("section"), lax.axis_index("tensor"), lax.axis_index("dp")
    size_t, size_d = lax.axis_size("tensor"), lax.axis_size("dp")
    group_index = section * size_t + tensor
    local_rows, width = att_ref.shape
    block, cols = mid.shape
    total_rows = att_all.shape[0]
    features = rows_ref.shape[1]
    chunks = gu.shape[0]
    dps = others("dp")
    sends = []

    loads = [
        pltpu.make_async_copy(wo_hbm.at[:, pl.ds(pl.multiple_of(me * cols, cols), cols)], wo, sem_w.at[0]),
        pltpu.make_async_copy(wg_hbm, wg, sem_w.at[1]),
        pltpu.make_async_copy(wu_hbm, wu, sem_w.at[2]),
        pltpu.make_async_copy(wd_hbm, wd, sem_w.at[3]),
    ]
    for load in loads:
        load.start()

    greet(group_peers() + [{"dp": to} for _, to, _ in dps])

    def dp_rows(index):
        return pl.ds(pl.multiple_of(index * local_rows, local_rows), local_rows)

    for step, to, _ in dps:
        copy = push(att_ref, att_all.at[dp_rows(me)], sem_att, step - 1, {"dp": to})
        copy.start()
        sends.append(copy)

    per = local_rows // block
    holder = group_index // per
    held_rows = pl.ds(pl.multiple_of(lax.rem(group_index, per) * block, block), block)

    def resid_copy(step, to):
        src = rows_ref.at[held_rows, pl.ds(pl.multiple_of(to * cols, cols), cols)]
        return push(src, resid, sem_res, step - 1, {"dp": to})

    @pl.when(me == holder)
    def _():
        for step, to, _ in dps:
            resid_copy(step, to).start()
        resid[...] = rows_ref[held_rows, pl.ds(pl.multiple_of(me * cols, cols), cols)]

    att_all[dp_rows(me), :] = att_ref[...]
    loads[0].wait()
    tile = tile_of(cols, 512)

    def out_part(index):
        lines = att_all[dp_rows(index), :]

        @pl.loop(0, cols // tile)
        def _(j):
            at = pl.ds(pl.multiple_of(j * tile, tile), tile)
            part[dp_rows(index), at] = jnp.dot(lines, wo[:, at], preferred_element_type=F32).astype(BF16)

    out_part(me)
    for step, to, source in dps:
        push(att_ref, att_all.at[dp_rows(source)], sem_att, step - 1, {"dp": to}).wait_recv()
        out_part(source)

    summed = scatter_group(part, pair_rx, comb, z_rx, sem_p, sem_z)

    for step, to, source in dps:
        @pl.when(source == holder)
        def _():
            resid_copy(step, to).wait_recv()

    @pl.when(me == holder)
    def _():
        for step, to, _ in dps:
            resid_copy(step, to).wait_send()

    mid_rows = (resid[...].astype(F32) + summed).astype(BF16)
    mid[...] = mid_rows
    squares = mid_rows.astype(F32)
    stat = jnp.sum(squares * squares, axis=-1, keepdims=True)
    stat_tx[...] = jnp.broadcast_to(stat, stat_tx.shape)
    for step, to, _ in dps:
        copy = push(stat_tx, stat_rx.at[step - 1], sem_stat, step - 1, {"dp": to})
        copy.start()
        sends.append(copy)
    for step, to, _ in dps:
        push(stat_tx, stat_rx.at[step - 1], sem_stat, step - 1, {"dp": to}).wait_recv()
        stat = stat + stat_rx[step - 1][:, :1]
    factor = lax.rsqrt(stat * (1.0 / features) + EPS)

    def token_rows(s, t):
        return pl.ds(pl.multiple_of((s * size_t + t) * block, block), block)

    nrm[token_rows(section, tensor), :] = (
        mid[...].astype(F32) * factor * gain_ref[...].astype(F32)
    ).astype(BF16)
    gather_group(nrm, token_rows, sem_t, sem_s)

    loads[1].wait()
    loads[2].wait()
    share = gu.shape[2] // 2
    gtile = tile_of(share, 256)
    square = size_d == 4
    if square:
        x, y = lax.rem(me, 2), me // 2
        near = [y * 2 + (1 - x), (1 - y) * 2 + x]
        far = (1 - y) * 2 + (1 - x)
    for c in range(chunks):
        @pl.loop(0, share // gtile)
        def _(j):
            src = pl.ds(pl.multiple_of(c * share + j * gtile, gtile), gtile)
            lo = pl.ds(pl.multiple_of(j * gtile, gtile), gtile)
            hi = pl.ds(pl.multiple_of(share + j * gtile, gtile), gtile)
            gu[c, :, lo] = jnp.dot(nrm[...], wg[:, src], preferred_element_type=F32).astype(BF16)
            gu[c, :, hi] = jnp.dot(nrm[...], wu[:, src], preferred_element_type=F32).astype(BF16)

        if square:
            first = near[c % 2]
            for slot, owner in ((1, far), (0, first)):
                copy = push(gu.at[c, dp_rows(owner)], rx1.at[c, slot], sem_1, 2 * c + slot, {"dp": first})
                copy.start()
                sends.append(copy)
        else:
            for step, to, _ in dps:
                slot = step - 1
                copy = push(gu.at[c, dp_rows(to)], rx1.at[c, slot], sem_1, (size_d - 1) * c + slot, {"dp": to})
                copy.start()
                sends.append(copy)

    if square:
        for c in range(chunks):
            first, second = near[c % 2], near[1 - c % 2]
            push(gu.at[c, dp_rows(far)], rx1.at[c, 1], sem_1, 2 * c + 1, {"dp": first}).wait_recv()
            tx2[c] = (gu[c, dp_rows(second), :].astype(F32) + rx1[c, 1].astype(F32)).astype(BF16)
            copy = push(tx2.at[c], rx2.at[c], sem_2, c, {"dp": second})
            copy.start()
            sends.append(copy)

    hid_slots = size_d - 1
    for c in range(chunks):
        both = gu[c, dp_rows(me), :].astype(F32)
        if square:
            first, second = near[c % 2], near[1 - c % 2]
            push(gu.at[c, dp_rows(first)], rx1.at[c, 0], sem_1, 2 * c, {"dp": first}).wait_recv()
            push(tx2.at[c], rx2.at[c], sem_2, c, {"dp": second}).wait_recv()
            both = both + rx1[c, 0].astype(F32) + rx2[c].astype(F32)
        else:
            for step, to, _ in dps:
                slot = step - 1
                push(
                    gu.at[c, dp_rows(to)], rx1.at[c, slot], sem_1, (size_d - 1) * c + slot, {"dp": to}
                ).wait_recv()
                both = both + rx1[c, slot].astype(F32)
        gate, up = both[:, :share], both[:, share:]
        hid[c, dp_rows(me), :] = (gate / (1.0 + jnp.exp(-gate)) * up).astype(BF16)
        mine = hid.at[c, dp_rows(me)]
        targets = list(enumerate(near)) if square else [(step - 1, to) for step, to, _ in dps]
        for slot, to in targets:
            copy = push(mine, mine, sem_h, hid_slots * c + slot, {"dp": to})
            copy.start()
            sends.append(copy)

    if square:
        for c in range(chunks):
            one, two = c % 2, 1 - c % 2
            theirs = hid.at[c, dp_rows(near[one])]
            push(theirs, theirs, sem_h, hid_slots * c + one, {"dp": near[one]}).wait_recv()
            copy = push(theirs, theirs, sem_h, hid_slots * c + 2, {"dp": near[two]})
            copy.start()
            sends.append(copy)

    loads[3].wait()
    for c in range(chunks):
        if square:
            two = 1 - c % 2
            arrivals = [(two, near[two]), (2, far)]
        else:
            arrivals = [(step - 1, source) for step, _, source in dps]
        for slot, source in arrivals:
            theirs = hid.at[c, dp_rows(source)]
            push(theirs, theirs, sem_h, hid_slots * c + slot, {"dp": source}).wait_recv()

        @pl.loop(0, cols // tile)
        def _(j):
            at = pl.ds(pl.multiple_of(j * tile, tile), tile)
            term = jnp.dot(hid[c], wd[c * share : (c + 1) * share, at], preferred_element_type=F32)
            if c > 0:
                term = acc[:, at] + term
            if c < chunks - 1:
                acc[:, at] = term
            else:
                part2[:, at] = term.astype(BF16)

    total = scatter_group(part2, pair_rx2, comb2, z_rx2, sem_p2, sem_z2)
    out_ref[...] = (mid[...].astype(F32) + total).astype(BF16)
    for copy in sends:
        copy.wait_send()


def back(attended, full_rows, gain, w_out, w_gate, w_up, w_down, collective_id):
    size_s, size_t, size_d = lax.axis_size("section"), lax.axis_size("tensor"), lax.axis_size("dp")
    local_rows, width = attended.shape
    total_rows = local_rows * size_d
    block = total_rows // (size_s * size_t)
    cols, hidden = w_gate.shape
    chunks = min(CHUNKS, hidden // 128)
    share = hidden // chunks
    slots = 2 if size_d == 4 else size_d - 1
    scatter = [
        pltpu.VMEM((total_rows, cols), BF16),
        pltpu.VMEM((size_s - 1, size_t, block, cols), BF16),
        pltpu.VMEM((size_t - 1, block, cols), BF16),
        pltpu.VMEM((size_t - 1, block, cols), BF16),
    ]
    return pl.pallas_call(
        back_body,
        out_shape=jax.ShapeDtypeStruct((block, cols), BF16),
        in_specs=[VMEM, VMEM, VMEM, ANY, ANY, ANY, ANY],
        out_specs=VMEM,
        scratch_shapes=[
            pltpu.VMEM((width, cols), BF16),
            pltpu.VMEM(w_gate.shape, BF16),
            pltpu.VMEM(w_up.shape, BF16),
            pltpu.VMEM(w_down.shape, BF16),
            pltpu.VMEM((total_rows, width), BF16),
            *scatter,
            pltpu.VMEM((block, cols), BF16),
            pltpu.VMEM((block, cols), BF16),
            pltpu.VMEM((block, 128), F32),
            pltpu.VMEM((size_d - 1, block, 128), F32),
            pltpu.VMEM((total_rows, cols), BF16),
            pltpu.VMEM((chunks, total_rows, 2 * share), BF16),
            pltpu.VMEM((chunks, slots, local_rows, 2 * share), BF16),
            pltpu.VMEM((chunks, local_rows, 2 * share), BF16),
            pltpu.VMEM((chunks, local_rows, 2 * share), BF16),
            pltpu.VMEM((chunks, total_rows, share), BF16),
            pltpu.VMEM((total_rows, cols), F32),
            *scatter,
            pltpu.SemaphoreType.DMA((4,)),
            pltpu.SemaphoreType.DMA,
            dma_sems(size_d - 1),
            dma_sems(size_d - 1),
            dma_sems((size_s - 1) * size_t),
            dma_sems(size_t - 1),
            dma_sems(size_d - 1),
            dma_sems(size_t - 1),
            dma_sems(size_t * (size_s - 1)),
            dma_sems(chunks * slots),
            dma_sems(chunks),
            dma_sems(chunks * (size_d - 1)),
            dma_sems((size_s - 1) * size_t),
            dma_sems(size_t - 1),
        ],
        compiler_params=pltpu.CompilerParams(
            collective_id=collective_id, has_side_effects=True, vmem_limit_bytes=66000000
        ),
    )(attended, full_rows, gain, w_out, w_gate, w_up, w_down)


def shards(tokens_in, gain_attn, w_query, w_keyval, w_out, gain_mlp, w_gate, w_up, w_down):
    data_index = lax.axis_index("dp")
    local_rows, width = tokens_in.shape
    total_rows = local_rows * lax.axis_size("dp")
    half_dim = HD // 2
    frequency = THETA ** (-jnp.arange(half_dim, dtype=jnp.float32) * 2.0 / HD)
    angles = jnp.arange(total_rows, dtype=jnp.int32).astype(F32)[:, None] * frequency[None, :]
    cosine, sine = jnp.cos(angles), jnp.sin(angles)
    attended, full_rows = front(
        tokens_in,
        gain_attn.reshape(-1, 1, width),
        jnp.concatenate([cosine, cosine], axis=1),
        jnp.concatenate([-sine, sine], axis=1),
        w_query,
        w_keyval,
        1,
    )
    cols = w_gate.shape[0]
    gain = lax.dynamic_slice_in_dim(gain_mlp, data_index * cols, cols, 0)[None, :]
    return back(attended, full_rows, gain, w_out, w_gate, w_up, w_down, 2)


def solution(mesh):
    placed = (
        P("dp", ("section", "tensor")),
        P(),
        P(None, ("section", "tensor")),
        P(None, ("section", "tensor")),
        P(("section", "tensor"), None),
        P(),
        P("dp", ("section", "tensor")),
        P("dp", ("section", "tensor")),
        P(("section", "tensor"), "dp"),
    )
    return jax.shard_map(
        shards,
        mesh=mesh,
        in_specs=placed,
        out_specs=P(("section", "tensor"), "dp"),
        check_vma=False,
    )
```
